32 devices in a mesh: dp: 1 (over z), tp: 4 (over y), fsdp: 8 (over x, core).
Axes of the slice: x: 4, y: 4, z: 1, core: 2. Of those that a mesh axis runs over, the one named last changes fastest.
The devices are a block of a 4x4x8 slice.
Arguments:
- hidden: bfloat16 [8, 768, 4096], P(('dp', 'fsdp'))
- seq_lens: int32 [8], P(('dp', 'fsdp'))
- w_qkv: bfloat16 [2, 4096, 3, 32, 128], P(None, 'fsdp', None, 'tp')
- b_qkv: bfloat16 [2, 3, 4096], P(None, None, ('tp', 'fsdp'))
- w_proj: bfloat16 [2, 4096, 4096], P(None, ('tp', 'fsdp'))
- w_up: bfloat16 [2, 4096, 16384], P(None, 'fsdp', 'tp')
- b_up: bfloat16 [2, 16384], P(None, ('tp', 'fsdp'))
- w_down: bfloat16 [2, 16384, 4096], P(None, ('tp', 'fsdp'))
- b_resid: bfloat16 [2, 2, 4096], P(None, None, 'fsdp')
- ln_params: float32 [2, 4, 4096], P(None, None, 'fsdp')
Outputs:
- output: bfloat16 [8, 768, 4096], P(('dp', 'fsdp'))
All inputs are finite; a program needn't handle non-finite values.
Results may differ from the reference program's by a relative error of at most 0.0172451.
Values are sent between devices in bfloat16 or wider.
A program may use at most 768 MiB of HBM per device.

```python
import jax
import jax.numpy as jnp
from jax import lax

D_MODEL = 4096
N_HEADS = 32
SEQ_LEN = 768
BATCH_ROWS = 8
LAYERS = 2
HEAD_DIM = D_MODEL // N_HEADS
FF_DIM = 4 * D_MODEL


def setup_inputs(seed: int = 0, part: int = 0) -> dict:
    root_key = jax.random.key(seed)
    sub_keys = jax.random.split(root_key, 9)
    part_key = jax.random.fold_in(sub_keys[8], part)
    hid_key, len_key = jax.random.split(part_key)
    hidden = jax.random.normal(hid_key, (BATCH_ROWS, SEQ_LEN, D_MODEL), jnp.float32).astype(jnp.bfloat16)
    drawn_lens = jax.random.randint(len_key, (BATCH_ROWS,), SEQ_LEN // 4, SEQ_LEN + 1, jnp.int32)
    seq_lens = jnp.concatenate([jnp.array([SEQ_LEN, SEQ_LEN // 4], jnp.int32), drawn_lens[2:]])

    def normal_w(rng_key, shape, w_scale):
        return (jax.random.normal(rng_key, shape, jnp.float32) * w_scale).astype(jnp.bfloat16)

    qkv_scale = jnp.array([1.5, 1.5, 1.0], jnp.float32)[:, None, None]
    w_qkv = normal_w(sub_keys[0], (LAYERS, D_MODEL, 3, N_HEADS, HEAD_DIM), D_MODEL ** -0.5 * qkv_scale)
    b_qkv = normal_w(sub_keys[1], (LAYERS, 3, D_MODEL), 0.5)
    w_proj = normal_w(sub_keys[2], (LAYERS, D_MODEL, D_MODEL), D_MODEL ** -0.5)
    w_up = normal_w(sub_keys[3], (LAYERS, D_MODEL, FF_DIM), D_MODEL ** -0.5)
    b_up = normal_w(sub_keys[4], (LAYERS, FF_DIM), 0.5)
    w_down = normal_w(sub_keys[5], (LAYERS, FF_DIM, D_MODEL), FF_DIM ** -0.5)
    b_resid = normal_w(sub_keys[6], (LAYERS, 2, D_MODEL), 0.3)
    ln_base = jnp.array([1.0, 0.0, 1.0, 0.0], jnp.float32)[None, :, None]
    ln_params = ln_base + 0.3 * jax.random.normal(sub_keys[7], (LAYERS, 4, D_MODEL), jnp.float32)
    return dict(hidden=hidden, seq_lens=seq_lens, w_qkv=w_qkv, b_qkv=b_qkv, w_proj=w_proj, w_up=w_up, b_up=b_up, w_down=w_down, b_resid=b_resid, ln_params=ln_params)


def layer_norm(acts_in, ln_gain, ln_shift):
    as_f32 = acts_in.astype(jnp.float32)
    row_mean = jnp.mean(as_f32, axis=-1, keepdims=True)
    centered = as_f32 - row_mean
    row_var = jnp.mean(centered * centered, axis=-1, keepdims=True)
    return (centered * lax.rsqrt(row_var + 1e-5) * ln_gain + ln_shift).astype(jnp.bfloat16)


def one_layer(seq_row, length, layer_params):
    w_qkv, b_qkv, w_proj, w_up, b_up, w_down, b_resid, ln_params = layer_params
    normed = layer_norm(seq_row, ln_params[0], ln_params[1])
    qkv_out = jnp.dot(normed, w_qkv.reshape(D_MODEL, 3 * D_MODEL), preferred_element_type=jnp.float32)
    qkv_out = (qkv_out + b_qkv.reshape(3 * D_MODEL).astype(jnp.float32)).astype(jnp.bfloat16)
    qkv_out = qkv_out.reshape(SEQ_LEN, 3, N_HEADS, HEAD_DIM).astype(jnp.float32)
    scores = jnp.einsum('qhe,khe->hqk', qkv_out[:, 0], qkv_out[:, 1]) * HEAD_DIM ** -0.5
    positions = jnp.arange(SEQ_LEN)
    allowed = (positions[None, :] <= positions[:, None]) & (positions[None, :] < length)
    scores = jnp.where(allowed[None], scores, -1e30)
    attn_probs = jax.nn.softmax(scores, axis=-1).astype(jnp.bfloat16).astype(jnp.float32)
    context = jnp.einsum('hqk,khe->qhe', attn_probs, qkv_out[:, 2]).astype(jnp.bfloat16)
    attn_out = jnp.dot(context.reshape(SEQ_LEN, D_MODEL), w_proj, preferred_element_type=jnp.float32)
    mid_state = (seq_row.astype(jnp.float32) + attn_out + b_resid[0].astype(jnp.float32)).astype(jnp.bfloat16)
    normed_mid = layer_norm(mid_state, ln_params[2], ln_params[3])
    up_out = jnp.dot(normed_mid, w_up, preferred_element_type=jnp.float32) + b_up.astype(jnp.float32)
    hidden_up = jnp.maximum(up_out, 0.0).astype(jnp.bfloat16)
    down_out = jnp.dot(hidden_up, w_down, preferred_element_type=jnp.float32)
    return (mid_state.astype(jnp.float32) + down_out + b_resid[1].astype(jnp.float32)).astype(jnp.bfloat16)


def reference(hidden, seq_lens, w_qkv, b_qkv, w_proj, w_up, b_up, w_down, b_resid, ln_params):
    stacked = (w_qkv, b_qkv, w_proj, w_up, b_up, w_down, b_resid, ln_params)

    def one_row(row_item):
        seq_row, length = row_item

        def layer_step(state_row, layer_params):
            return one_layer(state_row, length, layer_params), None

        return lax.scan(layer_step, seq_row, stacked)[0]

    return lax.map(one_row, (hidden, seq_lens))
```

```python
import functools

import jax
import jax.numpy as jnp
from jax import lax
from jax.experimental import pallas as pl
from jax.experimental.pallas import tpu as pltpu
from jax.sharding import PartitionSpec as P

TAIL_CUTS = (3, 6)
TILE = 512
VMEM_LIMIT = 56 * 1024 * 1024


def normalize(as_f32, ln_gain, ln_shift):
    row_mean = jnp.mean(as_f32, axis=-1, keepdims=True)
    centered = as_f32 - row_mean
    row_var = jnp.mean(centered * centered, axis=-1, keepdims=True)
    return (centered * lax.rsqrt(row_var + 1e-5) * ln_gain + ln_shift).astype(jnp.bfloat16)


def matmul_body(layout, with_bias, relu, *refs):
    n_acts = len(layout)
    acts_refs, weight_ref, rest = refs[:n_acts], refs[n_acts], refs[n_acts + 1:]
    bias_ref, rest = (rest[0], rest[1:]) if with_bias else (None, rest)
    out_ref = rest[0]
    blocks, depth, cols = weight_ref.shape
    acts_ref = acts_refs[0]
    if n_acts > 1:
        acts_ref = rest[1]

        @pl.when(pl.program_id(0) == 0)
        def _():
            for ref, (row, col) in zip(acts_refs, layout):
                acts_ref[row:row + ref.shape[0], col:col + ref.shape[1]] = ref[...]

    total = jnp.dot(acts_ref[...], weight_ref[...].reshape(blocks * depth, cols), preferred_element_type=jnp.float32)
    if with_bias:
        total += bias_ref[...]
    if relu:
        total = jnp.maximum(total, 0.0)
    out_ref[...] = total.astype(out_ref.dtype)


def matmul(acts, layout, weights, bias=None, relu=False):
    blocks, depth, cols = weights.shape
    n_rows = max(row + piece.shape[0] for piece, (row, _) in zip(acts, layout))
    tile = min(TILE, cols)
    operands = list(acts) + [weights]
    in_specs = [pl.BlockSpec(piece.shape, lambda n: (0, 0)) for piece in acts] + [pl.BlockSpec((blocks, depth, tile), lambda n: (0, 0, n))]
    if bias is not None:
        operands.append(bias)
        in_specs.append(pl.BlockSpec((1, tile), lambda n: (0, n)))
    work = n_rows * blocks * depth
    return pl.pallas_call(
        functools.partial(matmul_body, tuple(layout), bias is not None, relu),
        out_shape=jax.ShapeDtypeStruct((n_rows, cols), jnp.bfloat16),
        grid=(cols // tile,),
        in_specs=in_specs,
        out_specs=pl.BlockSpec((n_rows, tile), lambda n: (0, n)),
        scratch_shapes=[pltpu.VMEM((n_rows, blocks * depth), jnp.bfloat16)] if len(acts) > 1 else [],
        compiler_params=pltpu.CompilerParams(dimension_semantics=('arbitrary',), vmem_limit_bytes=VMEM_LIMIT),
        cost_estimate=pl.CostEstimate(flops=2 * work * cols, bytes_accessed=2 * (work + blocks * depth * cols + n_rows * cols), transcendentals=0),
    )(*operands)


def assemble_body(layout, rows, first_ref, *refs):
    out_ref = refs[-1]
    for block in range(max(row for row, _ in layout) // rows + 1):
        @pl.when(pl.program_id(0) == block)
        def _():
            for ref, (row, col) in zip(refs, layout):
                if row == block * rows:
                    out_ref[:, col:col + ref.shape[1]] = ref[...]


def assemble(first, pieces, layout, n_rows, n_cols):
    rows = pieces[0].shape[0]
    n_blocks = n_rows // rows
    return pl.pallas_call(
        functools.partial(assemble_body, tuple(layout), rows),
        out_shape=jax.ShapeDtypeStruct((n_rows, n_cols), pieces[0].dtype),
        grid_spec=pltpu.PrefetchScalarGridSpec(
            num_scalar_prefetch=1,
            grid=(n_blocks,),
            in_specs=[pl.BlockSpec(piece.shape, lambda b, _: (0, 0)) for piece in pieces],
            out_specs=pl.BlockSpec((rows, n_cols), lambda b, first_ref: (lax.rem(first_ref[0] + b, n_blocks), 0)),
        ),
        compiler_params=pltpu.CompilerParams(dimension_semantics=('arbitrary',), vmem_limit_bytes=VMEM_LIMIT),
        cost_estimate=pl.CostEstimate(flops=n_rows * n_cols, bytes_accessed=4 * n_rows * n_cols, transcendentals=0),
    )(first, *pieces)


def attend_body(info_ref, q_ref, k_ref, v_ref, out_ref):
    rows, head_dim = q_ref.shape
    shift, length = info_ref[0], info_ref[1]
    scores = lax.dot_general(q_ref[...], k_ref[...], (((1,), (1,)), ((), ())), preferred_element_type=jnp.float32) * head_dim ** -0.5
    query = lax.broadcasted_iota(jnp.int32, (rows, 1), 0) + shift
    query = jnp.where(query >= rows, query - rows, query)
    key = lax.broadcasted_iota(jnp.int32, (1, rows), 1) + shift
    key = jnp.where(key >= rows, key - rows, key)
    limit = jnp.minimum(query, length - 1)
    scores = jnp.where(key <= limit, scores, -1e30)
    weights = jnp.exp(scores - jnp.max(scores, axis=1, keepdims=True))
    probs = (weights / jnp.sum(weights, axis=1, keepdims=True)).astype(jnp.bfloat16)
    out_ref[...] = jnp.dot(probs, v_ref[...], preferred_element_type=jnp.float32).astype(out_ref.dtype)


def attend(info, qkv, heads, head_dim):
    rows = qkv.shape[0]
    return pl.pallas_call(
        attend_body,
        out_shape=jax.ShapeDtypeStruct((rows, heads * head_dim), jnp.bfloat16),
        grid_spec=pltpu.PrefetchScalarGridSpec(
            num_scalar_prefetch=1,
            grid=(heads,),
            in_specs=[pl.BlockSpec((rows, head_dim), lambda h, _, part=part: (0, part * heads + h)) for part in range(3)],
            out_specs=pl.BlockSpec((rows, head_dim), lambda h, _: (0, h)),
        ),
        compiler_params=pltpu.CompilerParams(dimension_semantics=('arbitrary',), vmem_limit_bytes=VMEM_LIMIT),
        cost_estimate=pl.CostEstimate(flops=8 * heads * rows * rows * head_dim, bytes_accessed=8 * rows * heads * head_dim, transcendentals=heads * rows * rows),
    )(info, qkv, qkv, qkv)


def after(value, *earlier):
    return lax.optimization_barrier((value,) + earlier)[0]


def solution(mesh):
    rows_spec = P(('dp', 'fsdp'), None, None)
    in_specs = (rows_spec, P(('dp', 'fsdp')), P(None, 'fsdp', None, 'tp', None), P(None, None, ('tp', 'fsdp')), P(None, ('tp', 'fsdp'), None), P(None, 'fsdp', 'tp'), P(None, ('tp', 'fsdp')), P(None, ('tp', 'fsdp'), None), P(None, None, 'fsdp'), P(None, None, 'fsdp'))
    n_tp = mesh.shape['tp']
    n_fsdp = mesh.shape['fsdp']
    assert n_tp == 4
    to_next = [(i, (i + 1) % n_tp) for i in range(n_tp)]
    to_prev = [(i, (i - 1) % n_tp) for i in range(n_tp)]

    def send_next(block):
        return lax.ppermute(block, 'tp', to_next)

    def send_prev(block):
        return lax.ppermute(block, 'tp', to_prev)

    def reduce_scatter(part):
        rows = part.shape[0] // n_tp
        half = part.shape[1] // 2
        own, nxt, opp, prv = (part[r * rows:(r + 1) * rows] for r in range(n_tp))
        opp_left = send_next(opp[:, :half])
        opp_right = send_prev(opp[:, half:])
        nxt_right = send_next(nxt[:, half:])
        prv_left = send_prev(prv[:, :half])
        nxt_left = send_next((nxt[:, :half].astype(jnp.float32) + opp_left.astype(jnp.float32)).astype(jnp.bfloat16))
        prv_right = send_prev((prv[:, half:].astype(jnp.float32) + opp_right.astype(jnp.float32)).astype(jnp.bfloat16))
        own = own.astype(jnp.float32)
        left = own[:, :half] + prv_left.astype(jnp.float32) + nxt_left.astype(jnp.float32)
        right = own[:, half:] + nxt_right.astype(jnp.float32) + prv_right.astype(jnp.float32)
        return jnp.concatenate([left, right], axis=1)

    def all_gather_rows(block):
        rows, half = block.shape[0], block.shape[1] // 2
        left, right = block[:, :half], block[:, half:]
        prv_left = send_next(left)
        nxt_right = send_prev(right)
        prv_right = send_next(right)
        nxt_left = send_prev(left)
        opp_left = send_next(prv_left)
        opp_right = send_prev(nxt_right)
        pieces = [block, nxt_left, nxt_right, opp_left, opp_right, prv_left, prv_right]
        layout = [(0, 0), (rows, 0), (rows, half), (2 * rows, 0), (2 * rows, half), (3 * rows, 0), (3 * rows, half)]
        return pieces, layout

    def per_device(hidden, seq_lens, w_qkv, b_qkv, w_proj, w_up, b_up, w_down, b_resid, ln_params):
        n_layers, _, _, local_heads, head_dim = w_qkv.shape
        seq_len, width = hidden.shape[1], hidden.shape[2]
        rows = seq_len // n_tp
        last = n_layers - 1
        me = lax.axis_index('tp')
        info = jnp.stack([(me * rows).astype(jnp.int32), seq_lens[0]])

        def gather(piece):
            return lax.all_gather(piece, 'fsdp', axis=0)

        qkv_full, proj_full, up_full, down_full = [], [], [], []
        for layer_idx in range(n_layers):
            qkv_full.append(gather(w_qkv[layer_idx].reshape(w_qkv.shape[1], -1)))
            proj_full.append(gather(w_proj[layer_idx]))
            up_full.append(gather(w_up[layer_idx]))
            down_full.append([gather(chunk) for chunk in jnp.split(w_down[layer_idx], [w_down.shape[2] * cut // 8 for cut in TAIL_CUTS] if layer_idx == last else 1, axis=1)])

        small = [ln_params, b_resid, b_up[:, None], b_qkv]
        packed = jnp.concatenate([item.astype(jnp.float32).reshape(-1) for item in small])
        packed = lax.all_gather(packed, 'fsdp', axis=0)
        unpacked, offset = [], 0
        for item in small:
            piece = packed[:, offset:offset + item.size].reshape((n_fsdp,) + item.shape)
            offset += item.size
            unpacked.append(jnp.moveaxis(piece, 0, 2).reshape(item.shape[0], item.shape[1], n_fsdp * item.shape[2]))
        ln_full, resid_bias, up_bias, qkv_bias = unpacked

        sequence = hidden[0]
        doubled = jnp.concatenate([sequence, sequence], axis=0)
        rotated = lax.dynamic_slice_in_dim(doubled, me * rows, seq_len, axis=0)
        own_state = rotated[:rows]
        pieces, layout = [normalize(rotated.astype(jnp.float32), ln_full[0, 0], ln_full[0, 1])], [(0, 0)]
        final_pieces, final_layout = [], []
        for layer_idx in range(n_layers):
            qkv = matmul(pieces, layout, qkv_full[layer_idx], qkv_bias[layer_idx].reshape(1, -1))
            context = attend(info, qkv, local_heads, head_dim)
            attn_sum = reduce_scatter(matmul([context], [(0, 0)], proj_full[layer_idx]))
            mid_state = (own_state.astype(jnp.float32) + attn_sum + resid_bias[layer_idx, 0]).astype(jnp.bfloat16)
            normed_own = normalize(mid_state.astype(jnp.float32), ln_full[layer_idx, 2], ln_full[layer_idx, 3])
            pieces, layout = all_gather_rows(normed_own)
            hidden_up = matmul(pieces, layout, up_full[layer_idx], up_bias[layer_idx], relu=True)
            states, gathered, start = [], [], 0
            for weights in down_full[layer_idx]:
                part = matmul([after(hidden_up, *gathered)], [(0, 0)], weights)
                cols = slice(start, start + part.shape[1])
                state = (mid_state[:, cols].astype(jnp.float32) + reduce_scatter(part) + resid_bias[layer_idx, 1, cols]).astype(jnp.bfloat16)
                states.append(state)
                if layer_idx == last:
                    gathered, layout = all_gather_rows(state)
                    final_pieces += gathered
                    final_layout += [(row, start + col) for row, col in layout]
                start += part.shape[1]
            if layer_idx < last:
                own_state = states[0]
                normed_own = normalize(own_state.astype(jnp.float32), ln_full[layer_idx + 1, 0], ln_full[layer_idx + 1, 1])
                pieces, layout = all_gather_rows(normed_own)
        out = assemble(me.astype(jnp.int32).reshape(1), final_pieces, final_layout, seq_len, width)
        return out[None]

    return jax.shard_map(per_device, mesh=mesh, in_specs=in_specs, out_specs=rows_spec, check_vma=False)
```

```python
import functools

import jax
import jax.numpy as jnp
from jax import lax
from jax.experimental import pallas as pl
from jax.experimental.pallas import tpu as pltpu
from jax.sharding import PartitionSpec as P


SHARE = 4
TILE = 512
VMEM_LIMIT = 56 * 1024 * 1024


def normalize(as_f32, ln_gain, ln_shift):
    row_mean = jnp.mean(as_f32, axis=-1, keepdims=True)
    centered = as_f32 - row_mean
    row_var = jnp.mean(centered * centered, axis=-1, keepdims=True)
    return (centered * lax.rsqrt(row_var + 1e-5) * ln_gain + ln_shift).astype(jnp.bfloat16)


def matmul_body(layout, n_weights, with_bias, relu, starts_ref, *refs):
    n_acts = len(layout)
    acts_refs, weight_refs, rest = refs[:n_acts], refs[n_acts:n_acts + n_weights], refs[n_acts + n_weights:]
    bias_ref, rest = (rest[0], rest[1:]) if with_bias else (None, rest)
    out_ref = rest[0]
    acts_ref = acts_refs[0]
    if n_acts > 1:
        acts_ref = rest[1]

        @pl.when(pl.program_id(0) == 0)
        def _():
            for ref, (row, col) in zip(acts_refs, layout):
                acts_ref[row:row + ref.shape[0], col:col + ref.shape[1]] = ref[...]

    if n_weights == 1:
        blocks, depth, cols = weight_refs[0].shape
        total = jnp.dot(acts_ref[...], weight_refs[0][...].reshape(blocks * depth, cols), preferred_element_type=jnp.float32)
    else:
        total = None
        for i, ref in enumerate(weight_refs):
            depth = ref.shape[0]
            acts = acts_ref[:, pl.ds(pl.multiple_of(starts_ref[i], 128), depth)]
            term = jnp.dot(acts, ref[...], preferred_element_type=jnp.float32)
            total = term if total is None else total + term
    if with_bias:
        total += bias_ref[...]
    if relu:
        total = jnp.maximum(total, 0.0)
    out_ref[...] = total.astype(out_ref.dtype)


def matmul(acts, layout, weights, bias=None, relu=False):
    weights, starts = weights if isinstance(weights, tuple) else ([weights], jnp.zeros((1,), jnp.int32))
    cols = weights[0].shape[-1]
    n_rows = max(row + piece.shape[0] for piece, (row, _) in zip(acts, layout))
    depth = max(col + piece.shape[1] for piece, (_, col) in zip(acts, layout))
    tile = min(TILE, cols)
    operands = list(acts) + list(weights)
    in_specs = [pl.BlockSpec(piece.shape, lambda n, _: (0, 0)) for piece in acts]
    for piece in weights:
        in_specs.append(pl.BlockSpec(piece.shape[:-1] + (tile,), lambda n, _, lead=piece.ndim - 1: (0,) * lead + (n,)))
    if bias is not None:
        operands.append(bias)
        in_specs.append(pl.BlockSpec((1, tile), lambda n, _: (0, n)))
    return pl.pallas_call(
        functools.partial(matmul_body, tuple(layout), len(weights), bias is not None, relu),
        out_shape=jax.ShapeDtypeStruct((n_rows, cols), jnp.bfloat16),
        grid_spec=pltpu.PrefetchScalarGridSpec(
            num_scalar_prefetch=1,
            grid=(cols // tile,),
            in_specs=in_specs,
            out_specs=pl.BlockSpec((n_rows, tile), lambda n, _: (0, n)),
            scratch_shapes=[pltpu.VMEM((n_rows, depth), jnp.bfloat16)] if len(acts) > 1 else [],
        ),
        compiler_params=pltpu.CompilerParams(dimension_semantics=('arbitrary',), vmem_limit_bytes=VMEM_LIMIT),
        cost_estimate=pl.CostEstimate(flops=2 * n_rows * depth * cols, bytes_accessed=2 * (n_rows * depth + depth * cols + n_rows * cols), transcendentals=0),
    )(starts, *operands)


def assemble_body(layout, rows, first_ref, *refs):
    out_ref = refs[-1]
    for block in range(max(row for row, _ in layout) // rows + 1):
        @pl.when(pl.program_id(0) == block)
        def _():
            for ref, (row, col) in zip(refs, layout):
                if row == block * rows:
                    out_ref[:, col:col + ref.shape[1]] = ref[...]


def assemble(first, pieces, layout, n_rows, n_cols):
    rows = pieces[0].shape[0]
    n_blocks = n_rows // rows
    return pl.pallas_call(
        functools.partial(assemble_body, tuple(layout), rows),
        out_shape=jax.ShapeDtypeStruct((n_rows, n_cols), pieces[0].dtype),
        grid_spec=pltpu.PrefetchScalarGridSpec(
            num_scalar_prefetch=1,
            grid=(n_blocks,),
            in_specs=[pl.BlockSpec(piece.shape, lambda b, _: (0, 0)) for piece in pieces],
            out_specs=pl.BlockSpec((rows, n_cols), lambda b, first_ref: (lax.rem(first_ref[0] + b, n_blocks), 0)),
        ),
        compiler_params=pltpu.CompilerParams(dimension_semantics=('arbitrary',), vmem_limit_bytes=VMEM_LIMIT),
        cost_estimate=pl.CostEstimate(flops=n_rows * n_cols, bytes_accessed=4 * n_rows * n_cols, transcendentals=0),
    )(first, *pieces)


def attend_body(info_ref, q_ref, k_ref, v_ref, out_ref):
    rows, head_dim = q_ref.shape
    shift, length = info_ref[0], info_ref[1]
    scores = lax.dot_general(q_ref[...], k_ref[...], (((1,), (1,)), ((), ())), preferred_element_type=jnp.float32) * head_dim ** -0.5
    query = lax.broadcasted_iota(jnp.int32, (rows, 1), 0) + shift
    query = jnp.where(query >= rows, query - rows, query)
    key = lax.broadcasted_iota(jnp.int32, (1, rows), 1) + shift
    key = jnp.where(key >= rows, key - rows, key)
    limit = jnp.minimum(query, length - 1)
    scores = jnp.where(key <= limit, scores, -1e30)
    weights = jnp.exp(scores - jnp.max(scores, axis=1, keepdims=True))
    probs = (weights / jnp.sum(weights, axis=1, keepdims=True)).astype(jnp.bfloat16)
    out_ref[...] = jnp.dot(probs, v_ref[...], preferred_element_type=jnp.float32).astype(out_ref.dtype)


def attend(info, qkv, heads, head_dim):
    rows = qkv.shape[0]
    return pl.pallas_call(
        attend_body,
        out_shape=jax.ShapeDtypeStruct((rows, heads * head_dim), jnp.bfloat16),
        grid_spec=pltpu.PrefetchScalarGridSpec(
            num_scalar_prefetch=1,
            grid=(heads,),
            in_specs=[pl.BlockSpec((rows, head_dim), lambda h, _, part=part: (0, part * heads + h)) for part in range(3)],
            out_specs=pl.BlockSpec((rows, head_dim), lambda h, _: (0, h)),
        ),
        compiler_params=pltpu.CompilerParams(dimension_semantics=('arbitrary',), vmem_limit_bytes=VMEM_LIMIT),
        cost_estimate=pl.CostEstimate(flops=8 * heads * rows * rows * head_dim, bytes_accessed=8 * rows * heads * head_dim, transcendentals=heads * rows * rows),
    )(info, qkv, qkv, qkv)


def after(value, *earlier):
    return lax.optimization_barrier((value,) + earlier)[0]


def solution(mesh):
    rows_spec = P(('dp', 'fsdp'), None, None)
    in_specs = (rows_spec, P(('dp', 'fsdp')), P(None, 'fsdp', None, 'tp', None), P(None, None, ('tp', 'fsdp')), P(None, ('tp', 'fsdp'), None), P(None, 'fsdp', 'tp'), P(None, ('tp', 'fsdp')), P(None, ('tp', 'fsdp'), None), P(None, None, 'fsdp'), P(None, None, 'fsdp'))
    n_tp = mesh.shape['tp']
    n_fsdp = mesh.shape['fsdp']
    assert n_tp == 4 and n_fsdp == 8
    to_next = [(i, (i + 1) % n_tp) for i in range(n_tp)]
    to_prev = [(i, (i - 1) % n_tp) for i in range(n_tp)]

    to_right = [(i, (i + 2) % n_fsdp) for i in range(n_fsdp)]
    to_left = [(i, (i - 2) % n_fsdp) for i in range(n_fsdp)]
    siblings = [(i, i ^ 1) for i in range(n_fsdp)]

    def exchange(name, piece, go):
        piece = after(piece, go)
        with jax.named_scope(f'{name}_right'):
            left = lax.ppermute(piece, 'fsdp', to_right)
        with jax.named_scope(f'{name}_left'):
            right = lax.ppermute(piece, 'fsdp', to_left)
        return piece, left, right

    def forward(name, pieces, then):
        piece, left, right = lax.optimization_barrier((*pieces, then))[:3]
        depth = piece.shape[0]
        half = depth // 2
        f = lax.axis_index('fsdp')
        with jax.named_scope(f'{name}_fartop'):
            far_top = lax.ppermute(left[:half], 'fsdp', to_right)
        with jax.named_scope(f'{name}_farlow'):
            far_low = lax.ppermute(right[half:], 'fsdp', to_left)
        weights, starts = [], []
        for part, shift, row in ((piece, 0, 0), (left, -2, 0), (right, 2, 0), (far_top, 4, 0), (far_low, 4, half)):
            weights += [part, lax.ppermute(part, 'fsdp', siblings)]
            starts += [(at + shift) % n_fsdp * depth + row for at in (f, f ^ 1)]
        return weights, jnp.stack(starts).astype(jnp.int32)

    def send_next(block):
        return lax.ppermute(block, 'tp', to_next)

    def send_prev(block):
        return lax.ppermute(block, 'tp', to_prev)

    def reduce_scatter(part):
        rows = part.shape[0] // n_tp
        half = part.shape[1] // 2
        own, nxt, opp, prv = (part[r * rows:(r + 1) * rows] for r in range(n_tp))
        opp_left = send_next(opp[:, :half])
        opp_right = send_prev(opp[:, half:])
        nxt_right = send_next(nxt[:, half:])
        prv_left = send_prev(prv[:, :half])
        nxt_left = send_next((nxt[:, :half].astype(jnp.float32) + opp_left.astype(jnp.float32)).astype(jnp.bfloat16))
        prv_right = send_prev((prv[:, half:].astype(jnp.float32) + opp_right.astype(jnp.float32)).astype(jnp.bfloat16))
        own = own.astype(jnp.float32)
        left = own[:, :half] + prv_left.astype(jnp.float32) + nxt_left.astype(jnp.float32)
        right = own[:, half:] + nxt_right.astype(jnp.float32) + prv_right.astype(jnp.float32)
        return jnp.concatenate([left, right], axis=1)

    def all_gather_rows(block, name='last'):
        rows, half = block.shape[0], block.shape[1] // 2
        left, right = block[:, :half], block[:, half:]
        prv_left = send_next(left)
        nxt_right = send_prev(right)
        prv_right = send_next(right)
        nxt_left = send_prev(left)
        with jax.named_scope(f'{name}_far'):
            opp_left = send_next(prv_left)
            opp_right = send_prev(nxt_right)
        pieces = [block, nxt_left, nxt_right, opp_left, opp_right, prv_left, prv_right]
        layout = [(0, 0), (rows, 0), (rows, half), (2 * rows, 0), (2 * rows, half), (3 * rows, 0), (3 * rows, half)]
        return pieces, layout

    def per_device(hidden, seq_lens, w_qkv, b_qkv, w_proj, w_up, b_up, w_down, b_resid, ln_params):
        n_layers, _, _, local_heads, head_dim = w_qkv.shape
        seq_len, width = hidden.shape[1], hidden.shape[2]
        rows = seq_len // n_tp
        last = n_layers - 1
        me = lax.axis_index('tp')
        info = jnp.stack([(me * rows).astype(jnp.int32), seq_lens[0]])

        def gather(piece):
            return lax.all_gather(piece, 'fsdp', axis=0)

        cut_up = w_up.shape[2] * SHARE // 8
        cut_down = w_down.shape[2] // 2
        qkv_full, proj_full, up_full, down_full = [], [], [], []
        for layer_idx in range(n_layers):
            qkv_full.append(gather(w_qkv[layer_idx].reshape(w_qkv.shape[1], -1)))
            proj_full.append(gather(w_proj[layer_idx]))
            up_full.append(gather(w_up[layer_idx][:, :cut_up]))
            starts = (0,) if layer_idx < n_layers - 1 else (0, cut_down)
            down_full.append([gather(w_down[layer_idx][:, start:start + cut_down]) for start in starts])

        up_parts = exchange('up0', w_up[0][:, cut_up:], qkv_full[0])

        small = [ln_params, b_resid, b_up[:, None], b_qkv]
        packed = jnp.concatenate([item.astype(jnp.float32).reshape(-1) for item in small])
        packed = lax.all_gather(packed, 'fsdp', axis=0)
        unpacked, offset = [], 0
        for item in small:
            piece = packed[:, offset:offset + item.size].reshape((n_fsdp,) + item.shape)
            offset += item.size
            unpacked.append(jnp.moveaxis(piece, 0, 2).reshape(item.shape[0], item.shape[1], n_fsdp * item.shape[2]))
        ln_full, resid_bias, up_bias, qkv_bias = unpacked

        sequence = hidden[0]
        doubled = jnp.concatenate([sequence, sequence], axis=0)
        rotated = lax.dynamic_slice_in_dim(doubled, me * rows, seq_len, axis=0)
        own_state = rotated[:rows]
        pieces, layout = [normalize(rotated.astype(jnp.float32), ln_full[0, 0], ln_full[0, 1])], [(0, 0)]
        final_pieces, final_layout = [], []
        for layer_idx in range(n_layers):
            with jax.named_scope(f'qkv{layer_idx}'):
                qkv = matmul(pieces, layout, qkv_full[layer_idx], qkv_bias[layer_idx].reshape(1, -1))
            context = attend(info, qkv, local_heads, head_dim)
            with jax.named_scope(f'proj{layer_idx}'):
                attn_part = matmul([context], [(0, 0)], proj_full[layer_idx])
            if layer_idx == last:
                up_weights = forward(f'up{layer_idx}', up_parts, attn_part)
            attn_sum = reduce_scatter(attn_part)
            mid_state = (own_state.astype(jnp.float32) + attn_sum + resid_bias[layer_idx, 0]).astype(jnp.bfloat16)
            if layer_idx < last:
                up_weights = forward(f'up{layer_idx}', up_parts, mid_state)
                down_parts = exchange(f'down{layer_idx}', w_down[layer_idx][:, cut_down:], mid_state)
            normed_own = normalize(mid_state.astype(jnp.float32), ln_full[layer_idx, 2], ln_full[layer_idx, 3])
            pieces, layout = all_gather_rows(normed_own, f'mid{layer_idx}')
            with jax.named_scope(f'upleft{layer_idx}'):
                up_left = matmul(pieces, layout, up_full[layer_idx], up_bias[layer_idx, :, :cut_up], relu=True)
            with jax.named_scope(f'upright{layer_idx}'):
                up_right = matmul(pieces, layout, up_weights, up_bias[layer_idx, :, cut_up:], relu=True)
            hidden_up, hidden_layout = [up_left, up_right], [(0, 0), (0, cut_up)]
            if layer_idx < last:
                down_full[layer_idx].append(forward(f'down{layer_idx}', down_parts, up_left))
            states = []
            for weights, cols in zip(down_full[layer_idx], (slice(0, cut_down), slice(cut_down, width))):
                with jax.named_scope(f'downlater{layer_idx}' if states else f'downfirst{layer_idx}'):
                    part = matmul(hidden_up, hidden_layout, weights)
                state = (mid_state[:, cols].astype(jnp.float32) + reduce_scatter(part) + resid_bias[layer_idx, 1, cols]).astype(jnp.bfloat16)
                states.append(state)
                if layer_idx == last:
                    gathered, layout = all_gather_rows(state)
                    final_pieces += gathered
                    final_layout += [(row, cols.start + col) for row, col in layout]
                    hidden_up = [after(up_left, *gathered), up_right]
            if layer_idx < last:
                own_state = jnp.concatenate(states, axis=1)
                up_parts = exchange(f'up{layer_idx + 1}', w_up[layer_idx + 1][:, cut_up:], own_state)
                normed_own = normalize(own_state.astype(jnp.float32), ln_full[layer_idx + 1, 0], ln_full[layer_idx + 1, 1])
                pieces, layout = all_gather_rows(normed_own, f'out{layer_idx}')
        out = assemble(me.astype(jnp.int32).reshape(1), final_pieces, final_layout, seq_len, width)
        return out[None]

    return jax.shard_map(per_device, mesh=mesh, in_specs=in_specs, out_specs=rows_spec, check_vma=False)
```
